32 devices in a mesh: dp: 8 (over z, y), tensor: 4 (over x, core).
Axes of the slice: x: 2, y: 2, z: 4, core: 2. Of those that a mesh axis runs over, the one named last changes fastest.
Arguments:
- qkv: bfloat16 [3, 2048, 4096], P(None, 'dp', 'tensor'), may hold values from -6 to 6
- segment_ids: int32 [8, 4, 64], P('dp'), may hold values from 0 to 1, never falling along the last dimension, each value on 1 to 63 neighbouring positions
- out_weight: bfloat16 [4096, 4096], P(None, 'tensor'), may hold values from -0.09375 to 0.09375
- out_bias: bfloat16 [4096], replicated, may hold values from -3 to 3
- upstream: bfloat16 [2048, 4096], P(('dp', 'tensor')), may hold values from -6 to 6
- pre_act: bfloat16 [2048, 8192], P('dp', 'tensor'), may hold values from -6 to 6
- down_weight: bfloat16 [4096, 8192], P('dp', 'tensor'), may hold values from -0.0625 to 0.0625
Outputs:
- attention_out: float32 [2048, 4096], P(('dp', 'tensor'))
- act_grad: float32 [2048, 8192], P('dp', 'tensor')
- weight_grad: float32 [4096, 8192], P('dp', 'tensor')
The draws below stay inside these ranges and needn't reach their ends.
Inputs may be any that keep to these rules, and one draw needn't show every extreme that they name: `segment_ids`: within each pack the ids never fall; 2 images a pack, each of 1 to 63 tokens.
All inputs are finite; a program needn't handle non-finite values.
Results may differ from the reference program's by a relative error of at most 0.0055.
Values may be sent and summed in bfloat16 or wider, within the bound.
No kernel may reach another device: no remote copies, remote signals or barrier semaphores. Data moves between devices by JAX's collectives and lax.ppermute only.
A program may use at most 128 MiB of HBM per device.

```python
import math
import jax
import jax.numpy as jnp
import numpy as np
from jax import lax

D = 4096
HEADS = 32
HEAD = 128
FF = 8192
ROWS_DEV = 64
TOKENS = 256
BATCH = 2048
HD = 4096
IMG_PACK = 2
MOST_IMG = 63
N_DP = 8
N_TENSOR = 4


def draw_qkv(key, part):
    sample = jax.random.truncated_normal(key, -6.0, 6.0, (3, BATCH, HD), jnp.float32)
    return sample.astype(jnp.bfloat16)


def spiked(result, key, source, target, shards_of, factor):
    def block_of(dim):
        return (jnp.arange(result.shape[dim]) // (result.shape[dim] // shards_of)).reshape((-1,) + (1,) * (result.ndim - 1 - dim))

    near = jax.random.permutation(key, shards_of)[block_of(target)]
    far = (block_of(target) + shards_of // 2) % shards_of
    return jnp.where((block_of(source) == near) | (block_of(source) == far), factor * result, result)


def shard_levels(stream_key, extent, pieces, least, largest):
    loudness = 1.0
    for dim, parts in pieces:
        steps = jax.random.uniform(jax.random.fold_in(jax.random.fold_in(stream_key, 6), dim), (parts,), jnp.float32, least / len(pieces), largest / len(pieces))
        loudness = loudness * jnp.repeat(jnp.exp(steps), extent[dim] // parts).reshape((-1,) + (1,) * (len(extent) - 1 - dim))
    return loudness


def profile(number_of, total, limit, lean):
    weights = [(1 << 20) // math.isqrt(rank ** lean) + 1 for rank in range(2, number_of + 1)]
    surplus, given = total - limit - (number_of - 1), [1] * (number_of - 1)
    while surplus > 0:
        movable = [i for i in range(number_of - 1) if given[i] < limit]
        mass, remaining = sum([weights[i] for i in movable]), surplus
        for i in movable:
            addition = min(limit - given[i], max(1, remaining * weights[i] // mass), surplus)
            given[i] = given[i] + addition
            surplus = surplus - addition
    return np.array([limit] + given)


def uneven(stream_key, number_of, total, most, lean):
    if number_of == 2:
        one = jax.random.randint(stream_key, (), max(1, total - most), min(most, total - 1) + 1)
        return jnp.stack([one, total - one])
    lengths = jnp.asarray(profile(number_of, total, most, lean), jnp.int32)
    pairs = (number_of - 1) // 2
    donor, receiver = lengths[1:1 + 2 * pairs:2], lengths[2:2 + 2 * pairs:2]
    slack = jnp.minimum(donor - 1, most - receiver)
    passed = jax.random.randint(jax.random.fold_in(stream_key, 1), (pairs,), 0, 1 << 20) % (slack + 1)
    lengths = lengths.at[1:1 + 2 * pairs:2].set(donor - passed).at[2:2 + 2 * pairs:2].set(receiver + passed)
    return lengths[jax.random.permutation(jax.random.fold_in(stream_key, 2), number_of)]


def normal_values(own_key, dims, deviation, most, shards=(), kind=jnp.bfloat16):
    result = deviation * jax.random.normal(own_key, dims, jnp.float32)
    if shards:
        result = result * shard_levels(own_key, dims, shards, -0.22, 0.18)
    return jnp.clip(result, -most, most).astype(kind)


def noise_with(key, extent, spread, most, shards, heavy, kind=jnp.bfloat16):
    values = spread * jax.random.normal(key, extent, jnp.float32)
    if shards:
        values = values * shard_levels(key, extent, shards, -0.22, 0.18)
    return jnp.clip(spiked(values, jax.random.fold_in(key, 3), *heavy), -most, most).astype(kind)


def setup_inputs(seed: int = 0) -> dict:
    splits = jax.random.split(jax.random.key(seed), 8)
    return {
        "qkv": draw_qkv(jax.random.fold_in(splits[7], 71), 0),
        "segment_ids": jax.vmap(lambda own: jnp.searchsorted(jnp.cumsum(uneven(own, IMG_PACK, ROWS_DEV, MOST_IMG, 2)), jnp.arange(ROWS_DEV), side="right"))(jax.random.split(splits[1], N_DP * N_TENSOR)).reshape((N_DP, N_TENSOR, ROWS_DEV)).astype(jnp.int32),
        "out_weight": normal_values(splits[2], (D, HD), HD ** -0.5, 0.09375, ((1, 4),)),
        "out_bias": normal_values(splits[3], (D,), 0.5, 3.0),
        "upstream": noise_with(splits[4], (BATCH, D), 1.0, 6.0, ((0, 32),), (0, 1, 32, 2.75)),
        "pre_act": normal_values(splits[5], (BATCH, FF), 1.0, 6.0, ((0, 8), (1, 4))),
        "down_weight": normal_values(splits[6], (D, FF), FF ** -0.5, 0.0625, ((0, 8), (1, 4))),
    }


root_half = 1.0 / math.sqrt(2.0)
inv_root_tau = 1.0 / math.sqrt(2.0 * math.pi)

def gelu_exact(argument):
    return 0.5 * argument * (1.0 + lax.erf(argument * root_half))

def gelu_slope(argument):
    return 0.5 * (1.0 + lax.erf(argument * root_half)) + argument * jnp.exp(-0.5 * argument * argument) * inv_root_tau

def attend(bundle):
    queries, key_rows, value_rows, labels = bundle
    length = queries.shape[0]
    queries = queries.reshape(length, HEADS, HEAD).astype(jnp.float32)
    key_rows = key_rows.reshape(length, HEADS, HEAD).astype(jnp.float32)
    value_rows = value_rows.reshape(length, HEADS, HEAD).astype(jnp.float32)
    scores = jnp.einsum('qhd,khd->hqk', queries, key_rows) * (1.0 / math.sqrt(HEAD))
    pack_of = jnp.arange(length, dtype=jnp.int32) // ROWS_DEV
    same_image = ((labels[:, None] == labels[None, :]) & (pack_of[:, None] == pack_of[None, :]))[None]
    masked = jnp.where(same_image, scores, -1e+30)
    row_top = lax.optimization_barrier(jnp.max(masked, axis=2, keepdims=True))
    exponent = jnp.where(same_image, jnp.exp(masked - row_top), 0.0)
    weights = (exponent / lax.optimization_barrier(jnp.sum(exponent, axis=2, keepdims=True))).astype(jnp.bfloat16)
    context = jnp.einsum('hqk,khd->qhd', weights.astype(jnp.float32), value_rows)
    return context.reshape(length, HD).astype(jnp.bfloat16)

def reference(qkv, segment_ids, out_weight, out_bias, upstream, pre_act, down_weight):
    packed = qkv.reshape(3, N_DP, TOKENS, HD)
    labels = segment_ids.reshape(N_DP, TOKENS)
    context = lax.map(attend, (packed[0], packed[1], packed[2], labels))
    context = context.reshape(BATCH, HD)
    share = HD // N_TENSOR
    running = jnp.zeros((BATCH, D), jnp.float32)
    for member in range(N_TENSOR):
        ctx_part = context[:, member * share:(member + 1) * share]
        weight_part = out_weight[:, member * share:(member + 1) * share]
        partial_value = lax.dot_general(ctx_part, weight_part, (((1,), (1,)), ((), ())), preferred_element_type=jnp.float32)
        rounded = lax.optimization_barrier(partial_value.astype(jnp.bfloat16))
        running = running + rounded.astype(jnp.float32)
    attention_out = running + out_bias.astype(jnp.float32)
    hidden_grad = jnp.dot(upstream, down_weight, preferred_element_type=jnp.float32)
    preact = pre_act.astype(jnp.float32)
    act_grad = hidden_grad * gelu_slope(preact)
    activation = gelu_exact(preact).astype(jnp.bfloat16)
    weight_grad = lax.dot_general(upstream, activation, (((0,), (0,)), ((), ())), preferred_element_type=jnp.float32) / N_DP
    return (attention_out, act_grad, weight_grad)
```

```python
import math

import jax
import jax.numpy as jnp
from jax import lax
from jax.sharding import PartitionSpec as P

HEAD = 128
ROWS_DEV = 64


root_half = 1.0 / math.sqrt(2.0)
inv_root_tau = 1.0 / math.sqrt(2.0 * math.pi)
f32, bf16 = jnp.float32, jnp.bfloat16


def gelu_exact(argument):
    return 0.5 * argument * (1.0 + lax.erf(argument * root_half))


def gelu_slope(argument):
    return (
        0.5 * (1.0 + lax.erf(argument * root_half))
        + argument * jnp.exp(-0.5 * argument * argument) * inv_root_tau
    )


def attend(qkv, labels):
    length = qkv.shape[1]
    head_count = qkv.shape[2] // HEAD
    queries = qkv[0].reshape(length, head_count, HEAD)
    key_rows = qkv[1].reshape(length, head_count, HEAD)
    value_rows = qkv[2].reshape(length, head_count, HEAD)
    scores = jnp.einsum("qhd,khd->hqk", queries, key_rows, preferred_element_type=jnp.float32) * (
        1.0 / math.sqrt(HEAD)
    )
    pack_of = jnp.arange(length, dtype=jnp.int32) // ROWS_DEV
    same_image = ((labels[:, None] == labels[None, :]) & (pack_of[:, None] == pack_of[None, :]))[
        None
    ]
    masked = jnp.where(same_image, scores, -1e30)
    row_top = jnp.max(masked, axis=2, keepdims=True)
    exponent = jnp.where(same_image, jnp.exp(masked - row_top), 0.0)
    weights = (exponent / jnp.sum(exponent, axis=2, keepdims=True)).astype(jnp.bfloat16)
    context = jnp.einsum("hqk,khd->qhd", weights, value_rows, preferred_element_type=jnp.float32)
    return context.reshape(length, head_count * HEAD).astype(jnp.bfloat16)


def make_body(n_dp, n_tensor):
    line, cross = n_dp // 2, n_tensor // 2

    def line_perm(shift, keep=lambda z: True):
        pairs = []
        for z in range(line):
            if keep(z):
                for side in range(2):
                    pairs.append((2 * z + side, 2 * ((z + shift) % line) + side))
        return pairs

    def along_line(value, shift, keep=lambda z: True):
        return lax.ppermute(value, "dp", line_perm(shift, keep))

    def across_side(value):
        return lax.ppermute(value, "dp", [(i, i ^ 1) for i in range(n_dp)])

    def across_core(value):
        return lax.ppermute(value, "tensor", [(t, t ^ 1) for t in range(n_tensor)])

    def along_cross(value, shift):
        return lax.ppermute(
            value, "tensor", [(t, (t + 2 * shift) % n_tensor) for t in range(n_tensor)]
        )

    def place(own, other, index, axis):
        first = jnp.where(index == 0, own, other)
        second = jnp.where(index == 0, other, own)
        return jnp.concatenate([first, second], axis=axis)

    def body(qkv, segment_ids, out_weight, out_bias, upstream, pre_act, down_weight):
        dp = lax.axis_index("dp")
        z, side = dp // 2, dp % 2
        t = lax.axis_index("tensor")
        x, core = t // 2, t % 2
        mine, d_model = upstream.shape
        tokens, hidden = pre_act.shape
        d_line = d_model // line
        d_side = d_line // 2
        half = hidden // 2

        pieces = []
        for k in range(line):
            columns = lax.dynamic_slice(
                upstream, (0, ((z + k) % line) * d_line), (mine, d_line)
            )
            pieces.append(columns if k == 0 else along_line(columns, k))
        grad = jnp.stack(pieces)
        grad = jnp.stack([grad, across_side(grad)], axis=1)
        by_cross = [grad] + [along_cross(grad, k) for k in range(1, cross)]
        if cross == 2:
            grad = place(by_cross[0][:, :, None], by_cross[1][:, :, None], x, 2)
        else:
            rolled = jnp.stack(by_cross, axis=2)
            grad = jnp.take(rolled, (x - jnp.arange(cross)) % cross, axis=2)
        grad = grad[:, :, :, None]
        grad = place(grad, across_core(grad), core, 3)
        grad = grad.reshape(line, 2 * tokens, d_line)

        preact = pre_act.astype(f32)
        activation = gelu_exact(preact).astype(bf16)
        keep_half = lax.dynamic_slice(activation, (0, side * half), (tokens, half))
        give_half = lax.dynamic_slice(activation, (0, (1 - side) * half), (tokens, half))
        chunk = jnp.concatenate([keep_half, across_side(give_half)], axis=0)

        stored_rows = down_weight.shape[0]
        w_keep = lax.dynamic_slice(down_weight, (0, side * half), (stored_rows, half))
        w_give = lax.dynamic_slice(down_weight, (0, (1 - side) * half), (stored_rows, half))
        weight = place(w_keep, across_side(w_give), side, 0)

        ups, downs = [], []
        right = left = chunk
        for s in range(1, line):
            right = along_line(right, 1, lambda z, s=s: s - 1 <= z < line - 1)
            left = along_line(left, -1, lambda z, s=s: 0 < z <= line - s)
            ups.append(right)
            downs.append(left)
        chunks = [chunk]
        for k in range(1, line):
            chunks.append(jnp.where(z >= k, ups[k - 1], downs[line - k - 1]))
        acts = jnp.stack(chunks)

        context = attend(qkv, segment_ids[0].reshape(-1))
        partial = lax.dot_general(
            context, out_weight, (((1,), (1,)), ((), ())), preferred_element_type=f32
        ).astype(bf16)
        share = partial.shape[0] // n_tensor
        total = lax.dynamic_slice(partial, (t * share, 0), (share, d_model)).astype(f32)
        for k in range(1, n_tensor):
            rows = lax.dynamic_slice(
                partial, (((t + k) % n_tensor) * share, 0), (share, d_model)
            )
            total = total + lax.ppermute(
                rows, "tensor", [(i, (i + k) % n_tensor) for i in range(n_tensor)]
            ).astype(f32)
        attention_out = total + out_bias.astype(f32)

        part = lax.dot_general(
            grad, weight, (((2,), (0,)), ((), ())), preferred_element_type=f32
        )
        going_right = going_left = None
        for s in range(1, line):
            out_right = part[s] if going_right is None else part[s] + going_right.astype(f32)
            out_left = (
                part[line - s] if going_left is None else part[line - s] + going_left.astype(f32)
            )
            going_right = along_line(out_right.astype(bf16), 1, lambda z, s=s: z < s and z < line - 1)
            going_left = along_line(out_left.astype(bf16), -1, lambda z, s=s: z > line - 1 - s and z > 0)
        summed = part[0] + going_right.astype(f32) + going_left.astype(f32)
        own_h = summed[:tokens]
        other_h = across_side(summed[tokens:].astype(bf16)).astype(f32)
        act_grad = place(own_h, other_h, side, 1) * gelu_slope(preact)

        product = lax.dot_general(
            grad.reshape(-1, d_line),
            acts.reshape(-1, half),
            (((0,), (0,)), ((), ())),
            preferred_element_type=f32,
        ) * (1.0 / n_dp)
        w_own = lax.dynamic_slice(product, (side * d_side, 0), (d_side, half))
        w_other = lax.dynamic_slice(product, ((1 - side) * d_side, 0), (d_side, half))
        weight_grad = place(w_own, across_side(w_other.astype(bf16)).astype(f32), side, 1)
        return (attention_out, act_grad, weight_grad)

    return body


def solution(mesh):
    return jax.shard_map(
        make_body(mesh.shape["dp"], mesh.shape["tensor"]),
        mesh=mesh,
        in_specs=(
            P(None, "dp", "tensor"),
            P("dp", None, None),
            P(None, "tensor"),
            P(),
            P(("dp", "tensor"), None),
            P("dp", "tensor"),
            P("dp", "tensor"),
        ),
        out_specs=(P(("dp", "tensor"), None), P("dp", "tensor"), P("dp", "tensor")),
        check_vma=False,
    )
```

```python
import math

import jax
import jax.numpy as jnp
from jax import lax
from jax.sharding import PartitionSpec as P


HEAD = 128
ROWS_DEV = 64


root_half = 1.0 / math.sqrt(2.0)
inv_root_tau = 1.0 / math.sqrt(2.0 * math.pi)
f32, bf16 = jnp.float32, jnp.bfloat16


def gelu_exact(argument):
    return 0.5 * argument * (1.0 + lax.erf(argument * root_half))


def gelu_slope(argument):
    return (
        0.5 * (1.0 + lax.erf(argument * root_half))
        + argument * jnp.exp(-0.5 * argument * argument) * inv_root_tau
    )


def attend(qkv, labels):
    length = qkv.shape[1]
    head_count = qkv.shape[2] // HEAD
    queries = qkv[0].reshape(length, head_count, HEAD)
    key_rows = qkv[1].reshape(length, head_count, HEAD)
    value_rows = qkv[2].reshape(length, head_count, HEAD)
    scores = jnp.einsum("qhd,khd->hqk", queries, key_rows, preferred_element_type=jnp.float32) * (
        1.0 / math.sqrt(HEAD)
    )
    pack_of = jnp.arange(length, dtype=jnp.int32) // ROWS_DEV
    same_image = ((labels[:, None] == labels[None, :]) & (pack_of[:, None] == pack_of[None, :]))[
        None
    ]
    masked = jnp.where(same_image, scores, -1e30)
    row_top = jnp.max(masked, axis=2, keepdims=True)
    exponent = jnp.where(same_image, jnp.exp(masked - row_top), 0.0)
    weights = (exponent / jnp.sum(exponent, axis=2, keepdims=True)).astype(jnp.bfloat16)
    context = jnp.einsum("hqk,khd->qhd", weights, value_rows, preferred_element_type=jnp.float32)
    return context.reshape(length, head_count * HEAD).astype(jnp.bfloat16)


def make_body(n_dp, n_tensor):
    line, cross = n_dp // 2, n_tensor // 2

    def along_line(value, shift, keep=lambda z: True):
        pairs = []
        for z in range(line):
            if keep(z):
                for side in range(2):
                    pairs.append((2 * z + side, 2 * ((z + shift) % line) + side))
        return lax.ppermute(value, "dp", pairs)

    def across_side(value):
        return lax.ppermute(value, "dp", [(i, i ^ 1) for i in range(n_dp)])

    def across_core(value):
        return lax.ppermute(value, "tensor", [(t, t ^ 1) for t in range(n_tensor)])

    def along_cross(value, shift):
        return lax.ppermute(
            value, "tensor", [(t, (t + 2 * shift) % n_tensor) for t in range(n_tensor)]
        )

    def place(own, other, index, axis):
        first = jnp.where(index == 0, own, other)
        second = jnp.where(index == 0, other, own)
        return jnp.concatenate([first, second], axis=axis)

    def body(qkv, segment_ids, out_weight, out_bias, upstream, pre_act, down_weight):
        dp = lax.axis_index("dp")
        z, side = dp // 2, dp % 2
        t = lax.axis_index("tensor")
        x, core = t // 2, t % 2
        mine, d_model = upstream.shape
        tokens, hidden = pre_act.shape
        d_line = d_model // line
        d_side = d_line // 2
        half = hidden // 2

        groups = [sorted({1, line - 1}), [*range(2, line - 1), 0]]
        shifted = []
        for k in [*groups[0], *groups[1]]:
            columns = lax.dynamic_slice(
                upstream, (0, ((z + k) % line) * d_line), (mine, d_line)
            )
            shifted.append(columns if k == 0 else along_line(columns, k))
        count = len(groups[0])
        grads = []
        for blocks in (shifted[:count], shifted[count:]):
            grad = jnp.stack(blocks)
            grad = jnp.stack([grad, across_side(grad)], axis=1)
            rolled = jnp.stack([grad] + [along_cross(grad, k) for k in range(1, cross)])
            swapped = across_core(rolled)
            placed = []
            for to_x in range(cross):
                for to_core in range(2):
                    value = None
                    for k in range(cross):
                        part = jnp.where(core == to_core, rolled[k], swapped[k])
                        value = (
                            part
                            if value is None
                            else jnp.where((x - to_x) % cross == k, part, value)
                        )
                    placed.append(value)
            grad = jnp.stack(placed, axis=2)
            grads.append(grad.reshape(len(blocks), 2, tokens, d_line))
        block_of = {}
        for g, blocks in enumerate(groups):
            for i, k in enumerate(blocks):
                block_of[k] = (g, i)

        preact = pre_act.astype(f32)
        activation, slope = lax.optimization_barrier(
            (gelu_exact(preact).astype(bf16), gelu_slope(preact))
        )
        quarter = half // 2
        acts = []
        for q in range(2):
            keep = lax.dynamic_slice(
                activation, (0, side * half + q * quarter), (tokens, quarter)
            )
            give = lax.dynamic_slice(
                activation, (0, (1 - side) * half + q * quarter), (tokens, quarter)
            )
            acts.append(jnp.concatenate([keep, across_side(give)], axis=0))

        stored_rows = down_weight.shape[0]
        w_keep = lax.dynamic_slice(down_weight, (0, side * half), (stored_rows, half))
        w_got = []
        for q in range(2):
            w_give = lax.dynamic_slice(
                down_weight,
                (q * (stored_rows // 2), (1 - side) * half),
                (stored_rows // 2, half),
            )
            w_got.append(across_side(w_give))
        weight = place(w_keep, jnp.concatenate(w_got, axis=0), side, 0)

        context = attend(qkv, segment_ids[0].reshape(-1))
        partial = lax.dot_general(
            context, out_weight, (((1,), (1,)), ((), ())), preferred_element_type=f32
        ).astype(bf16)
        share = partial.shape[0] // n_tensor
        total = lax.dynamic_slice(partial, (t * share, 0), (share, d_model)).astype(f32)
        for k in range(1, n_tensor):
            rows = lax.dynamic_slice(
                partial, (((t + k) % n_tensor) * share, 0), (share, d_model)
            )
            pairs = [(i, (i + k) % n_tensor) for i in range(n_tensor)]
            total = total + lax.ppermute(rows, "tensor", pairs).astype(f32)
        attention_out = total + out_bias.astype(f32)

        products = {}
        for g in range(2):
            for h in (1, 0):
                product = lax.dot_general(
                    grads[g][:, h], weight, (((2,), (0,)), ((), ())), preferred_element_type=f32
                )
                products[g, h] = lax.optimization_barrier(product)

        def part(k, h):
            g, i = block_of[k]
            return products[g, h][i]

        sums = {}
        for h in (1, 0):
            right = left = None
            for s in range(1, line):
                out_right, out_left = part(s, h), part(line - s, h)
                if right is not None:
                    out_right = out_right + right.astype(f32)
                    out_left = out_left + left.astype(f32)
                right = along_line(out_right.astype(bf16), 1, lambda p, s=s: p < s and p < line - 1)
                left = along_line(
                    out_left.astype(bf16), -1, lambda p, s=s: p > line - 1 - s and p > 0
                )
            sums[h] = part(0, h) + right.astype(f32) + left.astype(f32)
        other_h = across_side(sums[1].astype(bf16)).astype(f32)
        act_grad = place(sums[0], other_h, side, 1) * slope

        outs = []
        for q in range(2):
            ups, downs = [], []
            right = left = acts[q]
            for s in range(1, line):
                right = along_line(right, 1, lambda p, s=s: s - 1 <= p < line - 1)
                left = along_line(left, -1, lambda p, s=s: 0 < p <= line - s)
                ups.append(right)
                downs.append(left)
            product = None
            for g, blocks in enumerate(groups):
                chunk = jnp.concatenate(
                    [
                        acts[q] if k == 0 else jnp.where(z >= k, ups[k - 1], downs[line - k - 1])
                        for k in blocks
                    ],
                    axis=0,
                )
                term = lax.dot_general(
                    grads[g].reshape(-1, d_line),
                    chunk,
                    (((0,), (0,)), ((), ())),
                    preferred_element_type=f32,
                )
                product = term if product is None else product + term
            product = product * (1.0 / n_dp)
            own = lax.dynamic_slice(product, (side * d_side, 0), (d_side, quarter))
            other = lax.dynamic_slice(product, ((1 - side) * d_side, 0), (d_side, quarter))
            outs.append((own, across_side(other.astype(bf16)).astype(f32)))
        own = jnp.concatenate([o[0] for o in outs], axis=1)
        other = jnp.concatenate([o[1] for o in outs], axis=1)
        weight_grad = place(own, other, side, 1)
        return (attention_out, act_grad, weight_grad)

    return body


def solution(mesh):
    n_dp, n_tensor = mesh.shape["dp"], mesh.shape["tensor"]
    return jax.shard_map(
        make_body(n_dp, n_tensor),
        mesh=mesh,
        in_specs=(
            P(None, "dp", "tensor"),
            P("dp", None, None),
            P(None, "tensor"),
            P(),
            P(("dp", "tensor"), None),
            P("dp", "tensor"),
            P("dp", "tensor"),
        ),
        out_specs=(P(("dp", "tensor"), None), P("dp", "tensor"), P("dp", "tensor")),
        check_vma=False,
    )
```

```python
import math

import jax
import jax.numpy as jnp
from jax import lax
from jax.sharding import PartitionSpec as P


HEAD = 128
ROWS_DEV = 64


root_half = 1.0 / math.sqrt(2.0)
inv_root_tau = 1.0 / math.sqrt(2.0 * math.pi)
f32, bf16 = jnp.float32, jnp.bfloat16


def gelu_exact(argument):
    return 0.5 * argument * (1.0 + lax.erf(argument * root_half))


def gelu_slope(argument):
    return (
        0.5 * (1.0 + lax.erf(argument * root_half))
        + argument * jnp.exp(-0.5 * argument * argument) * inv_root_tau
    )


def attend(qkv, labels):
    length = qkv.shape[1]
    head_count = qkv.shape[2] // HEAD
    queries = qkv[0].reshape(length, head_count, HEAD)
    key_rows = qkv[1].reshape(length, head_count, HEAD)
    value_rows = qkv[2].reshape(length, head_count, HEAD)
    scores = jnp.einsum("qhd,khd->hqk", queries, key_rows, preferred_element_type=jnp.float32) * (
        1.0 / math.sqrt(HEAD)
    )
    pack_of = jnp.arange(length, dtype=jnp.int32) // ROWS_DEV
    same_image = ((labels[:, None] == labels[None, :]) & (pack_of[:, None] == pack_of[None, :]))[
        None
    ]
    masked = jnp.where(same_image, scores, -1e30)
    row_top = jnp.max(masked, axis=2, keepdims=True)
    exponent = jnp.where(same_image, jnp.exp(masked - row_top), 0.0)
    weights = (exponent / jnp.sum(exponent, axis=2, keepdims=True)).astype(jnp.bfloat16)
    context = jnp.einsum("hqk,khd->qhd", weights, value_rows, preferred_element_type=jnp.float32)
    return context.reshape(length, head_count * HEAD).astype(jnp.bfloat16)


STREAMS = 2


def make_body(n_dp, n_tensor):
    line, cross = n_dp // 2, n_tensor // 2

    def along_line(value, shift, keep=lambda z: True):
        pairs = []
        for z in range(line):
            if keep(z):
                for side in range(2):
                    pairs.append((2 * z + side, 2 * ((z + shift) % line) + side))
        return lax.ppermute(value, "dp", pairs)

    def across_side(value):
        return lax.ppermute(value, "dp", [(i, i ^ 1) for i in range(n_dp)])

    def across_core(value):
        return lax.ppermute(value, "tensor", [(t, t ^ 1) for t in range(n_tensor)])

    def along_cross(value, shift):
        return lax.ppermute(
            value, "tensor", [(t, (t + 2 * shift) % n_tensor) for t in range(n_tensor)]
        )

    def place(own, other, index, axis):
        first = jnp.where(index == 0, own, other)
        second = jnp.where(index == 0, other, own)
        return jnp.concatenate([first, second], axis=axis)

    def body(qkv, segment_ids, out_weight, out_bias, upstream, pre_act, down_weight):
        dp = lax.axis_index("dp")
        z, side = dp // 2, dp % 2
        t = lax.axis_index("tensor")
        x, core = t // 2, t % 2
        mine, d_model = upstream.shape
        tokens, hidden = pre_act.shape
        d_line = d_model // line
        d_side = d_line // 2
        half = hidden // 2

        def weight_grad_of(grads, act, ups, downs):
            product = None
            for g, blocks in enumerate(groups):
                chunk = jnp.concatenate(
                    [
                        act if k == 0 else jnp.where(z >= k, ups[k - 1], downs[line - k - 1])
                        for k in blocks
                    ],
                    axis=0,
                )
                term = lax.dot_general(
                    grads[g].reshape(-1, d_line),
                    chunk,
                    (((0,), (0,)), ((), ())),
                    preferred_element_type=f32,
                )
                product = term if product is None else product + term
            product = product * (1.0 / n_dp)
            own = lax.dynamic_slice(product, (side * d_side, 0), (d_side, width))
            other = lax.dynamic_slice(product, ((1 - side) * d_side, 0), (d_side, width))
            other = other.astype(bf16)
            return own, across_side(other)

        groups = [sorted({1, line - 1}), [*range(2, line - 1), 0]]
        shifted = []
        for k in [*groups[0], *groups[1]]:
            columns = lax.dynamic_slice(
                upstream, (0, ((z + k) % line) * d_line), (mine, d_line)
            )
            shifted.append(columns if k == 0 else along_line(columns, k))
        block_of = {k: (g, i) for g, blocks in enumerate(groups) for i, k in enumerate(blocks)}

        def gather_grad(g):
            blocks = shifted[: len(groups[0])] if g == 0 else shifted[len(groups[0]) :]
            grad = jnp.stack(blocks)
            grad = jnp.stack([grad, across_side(grad)], axis=1)
            got = [along_cross(grad, k) for k in range(1, cross)]
            rolled = jnp.stack([grad] + got)
            swapped = across_core(rolled)
            placed = []
            for to_x in range(cross):
                for to_core in range(2):
                    value = None
                    for k in range(cross):
                        part = jnp.where(core == to_core, rolled[k], swapped[k])
                        value = (
                            part
                            if value is None
                            else jnp.where((x - to_x) % cross == k, part, value)
                        )
                    placed.append(value)
            grad = jnp.stack(placed, axis=2)
            return grad.reshape(len(blocks), 2 * tokens, d_line)

        preact = pre_act.astype(f32)
        activation, slope = lax.optimization_barrier(
            (gelu_exact(preact).astype(bf16), gelu_slope(preact))
        )
        width = half // STREAMS
        acts = []
        for q in range(STREAMS):
            keep = lax.dynamic_slice(activation, (0, side * half + q * width), (tokens, width))
            give = lax.dynamic_slice(
                activation, (0, (1 - side) * half + q * width), (tokens, width)
            )
            acts.append(jnp.concatenate([keep, across_side(give)], axis=0))

        stored_rows = down_weight.shape[0]
        pieces = lax.optimization_barrier(
            [
                lax.dynamic_slice(down_weight, (0, s * half + q * width), (stored_rows, width))
                for q in range(STREAMS)
                for s in (side, 1 - side)
            ]
        )
        got_rows = [across_side(pieces[2 * q + 1]) for q in range(STREAMS)]

        weights, grads, products = [], [], {}

        def multiply(g, q):
            product = lax.dot_general(
                grads[g], weights[q], (((2,), (0,)), ((), ())), preferred_element_type=f32
            )
            products[g, q] = lax.optimization_barrier(product)

        grads.append(gather_grad(0))
        for q in range(STREAMS):
            weights.append(place(pieces[2 * q], got_rows[q], side, 0))
            multiply(0, q)
        grads.append(gather_grad(1))
        for q in range(STREAMS):
            multiply(1, q)

        def part(k, q):
            g, i = block_of[k]
            return products[g, q][i]

        moving = [(acts[q], acts[q]) for q in range(STREAMS)]
        ups, downs = [[] for _ in moving], [[] for _ in moving]
        outs, own_h, other_h = [], [], []
        for s in range(1, line + 1):
            for q in range(STREAMS):
                right, left = moving[q]
                if s > 1:
                    ups[q].append(right)
                    downs[q].append(left)
                    right = right.astype(f32) + jnp.where(z < s - 1, part(s - 1, q), 0.0)
                    left = left.astype(f32) + jnp.where(z > line - s, part(line - s + 1, q), 0.0)
                    right, left = right.astype(bf16), left.astype(bf16)
                if s == line:
                    outs.append(weight_grad_of(grads, acts[q], ups[q], downs[q]))
                right = along_line(right, 1, lambda p: p < line - 1)
                left = along_line(left, -1, lambda p: p > 0)
                moving[q] = right, left
        for q in range(STREAMS):
            right, left = moving[q]
            total = part(0, q) + right.astype(f32) + left.astype(f32)
            own_h.append(total[:tokens])
            give = total[tokens:].astype(bf16)
            other_h.append(across_side(give).astype(f32))
        act_grad = (
            place(jnp.concatenate(own_h, axis=1), jnp.concatenate(other_h, axis=1), side, 1)
            * slope
        )
        own = jnp.concatenate([o[0] for o in outs], axis=1)
        other = jnp.concatenate([o[1].astype(f32) for o in outs], axis=1)
        weight_grad = place(own, other, side, 1)

        qkv, _ = lax.optimization_barrier((qkv, products[0, 0]))
        context = attend(qkv, segment_ids[0].reshape(-1))
        partial = lax.dot_general(
            context, out_weight, (((1,), (1,)), ((), ())), preferred_element_type=f32
        ).astype(bf16)
        share = partial.shape[0] // n_tensor
        total = lax.dynamic_slice(partial, (t * share, 0), (share, d_model)).astype(f32)
        for k in range(1, n_tensor):
            rows = lax.dynamic_slice(
                partial, (((t + k) % n_tensor) * share, 0), (share, d_model)
            )
            pairs = [(i, (i + k) % n_tensor) for i in range(n_tensor)]
            total = total + lax.ppermute(rows, "tensor", pairs).astype(f32)
        attention_out = total + out_bias.astype(f32)
        return (attention_out, act_grad, weight_grad)

    return body


def solution(mesh):
    n_dp, n_tensor = mesh.shape["dp"], mesh.shape["tensor"]
    return jax.shard_map(
        make_body(n_dp, n_tensor),
        mesh=mesh,
        in_specs=(
            P(None, "dp", "tensor"),
            P("dp", None, None),
            P(None, "tensor"),
            P(),
            P(("dp", "tensor"), None),
            P("dp", "tensor"),
            P("dp", "tensor"),
        ),
        out_specs=(P(("dp", "tensor"), None), P("dp", "tensor"), P("dp", "tensor")),
        check_vma=False,
    )
```

```python
import math

import jax
import jax.numpy as jnp
from jax import lax
from jax.experimental import pallas as pl
from jax.experimental.pallas import tpu as pltpu
from jax.sharding import PartitionSpec as P


HEAD = 128
ROWS_DEV = 64


root_half = 1.0 / math.sqrt(2.0)
inv_root_tau = 1.0 / math.sqrt(2.0 * math.pi)
f32, bf16 = jnp.float32, jnp.bfloat16


def gelu_exact(argument):
    return 0.5 * argument * (1.0 + lax.erf(argument * root_half))


def gelu_slope(argument):
    return (
        0.5 * (1.0 + lax.erf(argument * root_half))
        + argument * jnp.exp(-0.5 * argument * argument) * inv_root_tau
    )


def attend_kernel(place_ref, qkv_ref, labels_ref, weight_ref, *refs):
    outs, (context, rolled) = refs[:-2], refs[-2:]
    length, width = context.shape
    share = length // len(outs)

    @pl.when(pl.program_id(0) == 0)
    def _():
        row = jnp.broadcast_to(labels_ref[...].astype(f32), (length, length))
        first = lax.broadcasted_iota(jnp.int32, (length, length), 0) // ROWS_DEV
        second = lax.broadcasted_iota(jnp.int32, (length, length), 1) // ROWS_DEV
        same = (row == row.T) & (first == second)
        for h in range(width // HEAD):
            cols = slice(h * HEAD, (h + 1) * HEAD)
            scores = lax.dot_general(
                qkv_ref[0, :, cols],
                qkv_ref[1, :, cols],
                (((1,), (1,)), ((), ())),
                preferred_element_type=f32,
            ) * (1.0 / math.sqrt(HEAD))
            masked = jnp.where(same, scores, -1e30)
            top = jnp.max(masked, axis=1, keepdims=True)
            exponent = jnp.where(same, jnp.exp(masked - top), 0.0)
            weights = (exponent / jnp.sum(exponent, axis=1, keepdims=True)).astype(bf16)
            context[:, cols] = jnp.dot(
                weights, qkv_ref[2, :, cols], preferred_element_type=f32
            ).astype(bf16)
        for k in range(len(outs)):
            start = pl.multiple_of(lax.rem(place_ref[0] + k, len(outs)) * share, share)
            rolled[k * share : (k + 1) * share, :] = context[pl.ds(start, share), :]

    partial = lax.dot_general(
        rolled[...], weight_ref[...], (((1,), (1,)), ((), ())), preferred_element_type=f32
    )
    for k, out in enumerate(outs):
        out[...] = partial[k * share : (k + 1) * share].astype(bf16)


def attend(qkv, labels, out_weight, place, members):
    length, width = qkv.shape[1:]
    d_model = out_weight.shape[0]
    block = min(512, d_model)
    share = length // members
    grid_spec = pltpu.PrefetchScalarGridSpec(
        num_scalar_prefetch=1,
        grid=(d_model // block,),
        in_specs=[
            pl.BlockSpec(qkv.shape, lambda j, p: (0, 0, 0)),
            pl.BlockSpec((1, length), lambda j, p: (0, 0)),
            pl.BlockSpec((block, width), lambda j, p: (j, 0)),
        ],
        out_specs=[pl.BlockSpec((share, block), lambda j, p: (0, j))] * members,
        scratch_shapes=[pltpu.VMEM((length, width), bf16)] * 2,
    )
    return pl.pallas_call(
        attend_kernel,
        grid_spec=grid_spec,
        out_shape=[jax.ShapeDtypeStruct((share, d_model), bf16)] * members,
        cost_estimate=pl.CostEstimate(
            flops=2 * length * width * (d_model + 2 * length),
            transcendentals=length * length * width // HEAD,
            bytes_accessed=2 * (qkv.size + out_weight.size + length * d_model),
        ),
        name="attend",
    )(place.reshape(1), qkv, labels.reshape(1, length), out_weight)


def merge_weight(index, products, others):
    rows, width = others[0].shape
    streams = len(others)
    steps = max(1, rows // 128)
    step = rows // steps

    def kernel(index_ref, *refs):
        out = refs[-1]
        for q in range(streams):
            mine = refs[q][...]
            theirs = refs[streams + q][...].astype(f32)
            low = slice(q * width, (q + 1) * width)
            high = slice((streams + q) * width, (streams + q + 1) * width)

            @pl.when(index_ref[0] == 0)
            def _():
                out[:, low] = mine
                out[:, high] = theirs

            @pl.when(index_ref[0] != 0)
            def _():
                out[:, low] = theirs
                out[:, high] = mine

    return pl.pallas_call(
        kernel,
        grid_spec=pltpu.PrefetchScalarGridSpec(
            num_scalar_prefetch=1,
            grid=(steps,),
            in_specs=[pl.BlockSpec((step, width), lambda i, n: (n[0] * steps + i, 0))] * streams
            + [pl.BlockSpec((step, width), lambda i, n: (i, 0))] * streams,
            out_specs=pl.BlockSpec((step, 2 * streams * width), lambda i, n: (i, 0)),
        ),
        out_shape=jax.ShapeDtypeStruct((rows, 2 * streams * width), f32),
        name="merge_weight",
    )(index, *products, *others)


def merge_act(index, own, others, slope):
    rows, width = others[0].shape
    streams = len(others)
    steps = max(1, rows // 128)
    step = rows // steps

    def kernel(index_ref, *refs):
        factor, out = refs[-2], refs[-1]
        for q in range(streams):
            mine = refs[q][...]
            theirs = refs[streams + q][...].astype(f32)
            low = slice(q * width, (q + 1) * width)
            high = slice((streams + q) * width, (streams + q + 1) * width)

            @pl.when(index_ref[0] == 0)
            def _():
                out[:, low] = mine * factor[:, low]
                out[:, high] = theirs * factor[:, high]

            @pl.when(index_ref[0] != 0)
            def _():
                out[:, low] = theirs * factor[:, low]
                out[:, high] = mine * factor[:, high]

    block = pl.BlockSpec((step, width), lambda i, n: (i, 0))
    wide = pl.BlockSpec((step, 2 * streams * width), lambda i, n: (i, 0))
    return pl.pallas_call(
        kernel,
        grid_spec=pltpu.PrefetchScalarGridSpec(
            num_scalar_prefetch=1,
            grid=(steps,),
            in_specs=[block] * (2 * streams) + [wide],
            out_specs=wide,
        ),
        out_shape=jax.ShapeDtypeStruct(slope.shape, f32),
        name="merge_act",
    )(index, *own, *others, slope)


STREAMS = 2


def make_body(n_dp, n_tensor):
    line, cross = n_dp // 2, n_tensor // 2

    def along_line(value, shift, keep=lambda z: True):
        pairs = []
        for z in range(line):
            if keep(z):
                for side in range(2):
                    pairs.append((2 * z + side, 2 * ((z + shift) % line) + side))
        return lax.ppermute(value, "dp", pairs)

    def across_side(value):
        return lax.ppermute(value, "dp", [(i, i ^ 1) for i in range(n_dp)])

    def across_core(value):
        return lax.ppermute(value, "tensor", [(t, t ^ 1) for t in range(n_tensor)])

    def along_cross(value, shift):
        return lax.ppermute(
            value, "tensor", [(t, (t + 2 * shift) % n_tensor) for t in range(n_tensor)]
        )

    def place(own, other, index, axis):
        first = jnp.where(index == 0, own, other)
        second = jnp.where(index == 0, other, own)
        return jnp.concatenate([first, second], axis=axis)

    def body(qkv, segment_ids, out_weight, out_bias, upstream, pre_act, down_weight):
        dp = lax.axis_index("dp")
        z, side = dp // 2, dp % 2
        t = lax.axis_index("tensor")
        x, core = t // 2, t % 2
        mine, d_model = upstream.shape
        tokens, hidden = pre_act.shape
        d_line = d_model // line
        d_side = d_line // 2
        half = hidden // 2

        def first_then(first, then):
            return lax.optimization_barrier((then, first))[0]

        def weight_grad_of(grads, act, ups, downs):
            product = None
            for g, blocks in enumerate(groups):
                chunk = jnp.concatenate(
                    [
                        act if k == 0 else jnp.where(z >= k, ups[k - 1], downs[line - k - 1])
                        for k in blocks
                    ],
                    axis=0,
                )
                term = lax.dot_general(
                    grads[g].reshape(-1, d_line),
                    chunk,
                    (((0,), (0,)), ((), ())),
                    preferred_element_type=f32,
                )
                product = term if product is None else product + term
            return product * (1.0 / n_dp)

        groups = [sorted({1, line - 1}), [*range(2, line - 1), 0]]
        shifted = []
        for k in [*groups[0], *groups[1]]:
            columns = lax.dynamic_slice(
                upstream, (0, ((z + k) % line) * d_line), (mine, d_line)
            )
            shifted.append(columns if k == 0 else along_line(columns, k))
        block_of = {k: (g, i) for g, blocks in enumerate(groups) for i, k in enumerate(blocks)}

        def gather_grad(g):
            blocks = shifted[: len(groups[0])] if g == 0 else shifted[len(groups[0]) :]
            grad = jnp.stack(blocks)
            grad = jnp.stack([grad, across_side(grad)], axis=1)
            got = [along_cross(grad, k) for k in range(1, cross)]
            rolled = jnp.stack([grad] + got)
            swapped = across_core(rolled)
            placed = []
            for to_x in range(cross):
                for to_core in range(2):
                    value = None
                    for k in range(cross):
                        part = jnp.where(core == to_core, rolled[k], swapped[k])
                        value = (
                            part
                            if value is None
                            else jnp.where((x - to_x) % cross == k, part, value)
                        )
                    placed.append(value)
            grad = jnp.stack(placed, axis=2)
            return grad.reshape(len(blocks), 2 * tokens, d_line)

        preact = pre_act.astype(f32)
        activation, slope = lax.optimization_barrier(
            (gelu_exact(preact).astype(bf16), gelu_slope(preact))
        )
        width = half // STREAMS
        keep = lax.dynamic_slice(activation, (0, side * half), (tokens, half))
        give = lax.dynamic_slice(activation, (0, (1 - side) * half), (tokens, half))
        act = jnp.concatenate([keep, across_side(give)], axis=0)

        stored_rows = down_weight.shape[0]
        pieces = lax.optimization_barrier(
            [
                lax.dynamic_slice(down_weight, (0, s * half + q * width), (stored_rows, width))
                for q in range(STREAMS)
                for s in (side, 1 - side)
            ]
        )
        got_rows = [across_side(pieces[2 * q + 1]) for q in range(STREAMS)]

        weights, grads, products = [], [], {}

        def multiply(g, q):
            product = lax.dot_general(
                grads[g], weights[q], (((2,), (0,)), ((), ())), preferred_element_type=f32
            )
            products[g, q] = lax.optimization_barrier(product)

        grads.append(gather_grad(0))
        for q in range(STREAMS):
            weights.append(place(pieces[2 * q], got_rows[q], side, 0))
            multiply(0, q)
        grads.append(gather_grad(1))
        for q in range(STREAMS):
            multiply(1, q)

        def part(k, q):
            g, i = block_of[k]
            return products[g, q][i]

        def slot(right, left):
            right = along_line(right, 1, lambda p: p < line - 1)
            left = along_line(left, -1, lambda p: p > 0)
            return right, left

        def of_stream(value, q):
            return value[:, q * width : (q + 1) * width]

        got = slot(act, act)
        moving = [tuple(of_stream(v, q) for v in got) for q in range(STREAMS)]
        ups, downs = [[] for _ in moving], [[] for _ in moving]
        index = side.reshape(1)
        full, others = [], []
        for s in range(2, line + 1):
            for q in range(STREAMS):
                right, left = moving[q]
                ups[q].append(right)
                downs[q].append(left)
                to_right, to_left = part(s - 1, q), part(line - s + 1, q)
                if s == 2 and q:
                    to_right, to_left = first_then(joined, (to_right, to_left))
                right = right.astype(f32) + jnp.where(z < s - 1, to_right, 0.0)
                left = left.astype(f32) + jnp.where(z > line - s, to_left, 0.0)
                joined = right, left = right.astype(bf16), left.astype(bf16)
                if s == line:
                    own_act = of_stream(act, q)
                    if q:
                        own_act, ups[q][0], downs[q][0] = first_then(
                            other, (own_act, ups[q][0], downs[q][0])
                        )
                    product = weight_grad_of(grads, own_act, ups[q], downs[q])
                    other = lax.dynamic_slice(
                        product, ((1 - side) * d_side, 0), (d_side, width)
                    ).astype(bf16)
                    others.append(across_side(other))
                    full.append(product)
                moving[q] = slot(right, left)
        own, gives = [], []
        for q in range(STREAMS):
            right, left = moving[q]
            total_h = part(0, q) + right.astype(f32) + left.astype(f32)
            own.append(total_h[:tokens])
            give = total_h[tokens:].astype(bf16)
            gives.append(across_side(give))
        weight_grad = merge_weight(index, full, others)
        act_grad = merge_act(index, own, gives, slope)

        shares = list(attend(qkv, segment_ids[0], out_weight, t, n_tensor))
        for k in range(1, n_tensor):
            pairs = [(i, (i + k) % n_tensor) for i in range(n_tensor)]
            shares[k] = lax.ppermute(shares[k], "tensor", pairs)
        attention_out = sum(share.astype(f32) for share in shares) + out_bias.astype(f32)
        return (attention_out, act_grad, weight_grad)

    return body


def solution(mesh):
    n_dp, n_tensor = mesh.shape["dp"], mesh.shape["tensor"]
    return jax.shard_map(
        make_body(n_dp, n_tensor),
        mesh=mesh,
        in_specs=(
            P(None, "dp", "tensor"),
            P("dp", None, None),
            P(None, "tensor"),
            P(),
            P(("dp", "tensor"), None),
            P("dp", "tensor"),
            P("dp", "tensor"),
        ),
        out_specs=(P(("dp", "tensor"), None), P("dp", "tensor"), P("dp", "tensor")),
        check_vma=False,
    )
```

```python
import math

import jax
import jax.numpy as jnp
from jax import lax
from jax.experimental import pallas as pl
from jax.experimental.pallas import tpu as pltpu
from jax.sharding import PartitionSpec as P


HEAD = 128
ROWS_DEV = 64


root_half = 1.0 / math.sqrt(2.0)
inv_root_tau = 1.0 / math.sqrt(2.0 * math.pi)
f32, bf16 = jnp.float32, jnp.bfloat16


def gelu_exact(argument):
    return 0.5 * argument * (1.0 + lax.erf(argument * root_half))


def gelu_slope(argument):
    return (
        0.5 * (1.0 + lax.erf(argument * root_half))
        + argument * jnp.exp(-0.5 * argument * argument) * inv_root_tau
    )


def attend_kernel(place_ref, qkv_ref, labels_ref, weight_ref, *refs):
    outs, (context, rolled) = refs[:-2], refs[-2:]
    length, width = context.shape
    share = length // len(outs)

    @pl.when(pl.program_id(0) == 0)
    def _():
        row = jnp.broadcast_to(labels_ref[...].astype(f32), (length, length))
        first = lax.broadcasted_iota(jnp.int32, (length, length), 0) // ROWS_DEV
        second = lax.broadcasted_iota(jnp.int32, (length, length), 1) // ROWS_DEV
        same = (row == row.T) & (first == second)
        for h in range(width // HEAD):
            cols = slice(h * HEAD, (h + 1) * HEAD)
            scores = lax.dot_general(
                qkv_ref[0, :, cols],
                qkv_ref[1, :, cols],
                (((1,), (1,)), ((), ())),
                preferred_element_type=f32,
            ) * (1.0 / math.sqrt(HEAD))
            masked = jnp.where(same, scores, -1e30)
            top = jnp.max(masked, axis=1, keepdims=True)
            exponent = jnp.where(same, jnp.exp(masked - top), 0.0)
            weights = (exponent / jnp.sum(exponent, axis=1, keepdims=True)).astype(bf16)
            context[:, cols] = jnp.dot(
                weights, qkv_ref[2, :, cols], preferred_element_type=f32
            ).astype(bf16)
        for k in range(len(outs)):
            start = pl.multiple_of(lax.rem(place_ref[0] + k, len(outs)) * share, share)
            rolled[k * share : (k + 1) * share, :] = context[pl.ds(start, share), :]

    partial = lax.dot_general(
        rolled[...], weight_ref[...], (((1,), (1,)), ((), ())), preferred_element_type=f32
    )
    for k, out in enumerate(outs):
        out[...] = partial[k * share : (k + 1) * share].astype(bf16)


def attend(qkv, labels, out_weight, place, members):
    length, width = qkv.shape[1:]
    d_model = out_weight.shape[0]
    block = min(512, d_model)
    share = length // members
    grid_spec = pltpu.PrefetchScalarGridSpec(
        num_scalar_prefetch=1,
        grid=(d_model // block,),
        in_specs=[
            pl.BlockSpec(qkv.shape, lambda j, p: (0, 0, 0)),
            pl.BlockSpec((1, length), lambda j, p: (0, 0)),
            pl.BlockSpec((block, width), lambda j, p: (j, 0)),
        ],
        out_specs=[pl.BlockSpec((share, block), lambda j, p: (0, j))] * members,
        scratch_shapes=[pltpu.VMEM((length, width), bf16)] * 2,
    )
    return pl.pallas_call(
        attend_kernel,
        grid_spec=grid_spec,
        out_shape=[jax.ShapeDtypeStruct((share, d_model), bf16)] * members,
        cost_estimate=pl.CostEstimate(
            flops=2 * length * width * (d_model + 2 * length),
            transcendentals=length * length * width // HEAD,
            bytes_accessed=2 * (qkv.size + out_weight.size + length * d_model),
        ),
        name="attend",
    )(place.reshape(1), qkv, labels.reshape(1, length), out_weight)


def merge_weight(index, products, others):
    rows, width = others[0].shape
    streams = len(others)
    steps = max(1, rows // 128)
    step = rows // steps

    def kernel(index_ref, *refs):
        out = refs[-1]
        for q in range(streams):
            mine = refs[q][...]
            theirs = refs[streams + q][...].astype(f32)
            low = slice(q * width, (q + 1) * width)
            high = slice((streams + q) * width, (streams + q + 1) * width)

            @pl.when(index_ref[0] == 0)
            def _():
                out[:, low] = mine
                out[:, high] = theirs

            @pl.when(index_ref[0] != 0)
            def _():
                out[:, low] = theirs
                out[:, high] = mine

    return pl.pallas_call(
        kernel,
        grid_spec=pltpu.PrefetchScalarGridSpec(
            num_scalar_prefetch=1,
            grid=(steps,),
            in_specs=[pl.BlockSpec((step, width), lambda i, n: (n[0] * steps + i, 0))] * streams
            + [pl.BlockSpec((step, width), lambda i, n: (i, 0))] * streams,
            out_specs=pl.BlockSpec((step, 2 * streams * width), lambda i, n: (i, 0)),
        ),
        out_shape=jax.ShapeDtypeStruct((rows, 2 * streams * width), f32),
        name="merge_weight",
    )(index, *products, *others)


def merge_act(index, own, others, slope):
    rows, width = others[0].shape
    streams = len(others)
    steps = max(1, rows // 128)
    step = rows // steps

    def kernel(index_ref, *refs):
        factor, out = refs[-2], refs[-1]
        for q in range(streams):
            mine = refs[q][...]
            theirs = refs[streams + q][...].astype(f32)
            low = slice(q * width, (q + 1) * width)
            high = slice((streams + q) * width, (streams + q + 1) * width)

            @pl.when(index_ref[0] == 0)
            def _():
                out[:, low] = mine * factor[:, low]
                out[:, high] = theirs * factor[:, high]

            @pl.when(index_ref[0] != 0)
            def _():
                out[:, low] = theirs * factor[:, low]
                out[:, high] = mine * factor[:, high]

    block = pl.BlockSpec((step, width), lambda i, n: (i, 0))
    wide = pl.BlockSpec((step, 2 * streams * width), lambda i, n: (i, 0))
    return pl.pallas_call(
        kernel,
        grid_spec=pltpu.PrefetchScalarGridSpec(
            num_scalar_prefetch=1,
            grid=(steps,),
            in_specs=[block] * (2 * streams) + [wide],
            out_specs=wide,
        ),
        out_shape=jax.ShapeDtypeStruct(slope.shape, f32),
        name="merge_act",
    )(index, *own, *others, slope)


STREAMS = 2


def make_body(n_dp, n_tensor):
    line, cross = n_dp // 2, n_tensor // 2

    def along_line(value, shift, keep=lambda z: True):
        pairs = []
        for z in range(line):
            if keep(z):
                for side in range(2):
                    pairs.append((2 * z + side, 2 * ((z + shift) % line) + side))
        return lax.ppermute(value, "dp", pairs)

    def across_side(value):
        return lax.ppermute(value, "dp", [(i, i ^ 1) for i in range(n_dp)])

    def across_core(value):
        return lax.ppermute(value, "tensor", [(t, t ^ 1) for t in range(n_tensor)])

    def along_cross(value, shift):
        return lax.ppermute(
            value, "tensor", [(t, (t + 2 * shift) % n_tensor) for t in range(n_tensor)]
        )

    def place(own, other, index, axis):
        first = jnp.where(index == 0, own, other)
        second = jnp.where(index == 0, other, own)
        return jnp.concatenate([first, second], axis=axis)

    def body(qkv, segment_ids, out_weight, out_bias, upstream, pre_act, down_weight):
        dp = lax.axis_index("dp")
        z, side = dp // 2, dp % 2
        t = lax.axis_index("tensor")
        x, core = t // 2, t % 2
        mine, d_model = upstream.shape
        tokens, hidden = pre_act.shape
        d_line = d_model // line
        d_side = d_line // 2
        half = hidden // 2

        def first_then(first, then):
            return lax.optimization_barrier((then, first))[0]

        def weight_grad_of(grads, act, ups, downs):
            product = None
            for g, blocks in enumerate(groups):
                chunk = jnp.concatenate(
                    [
                        act if k == 0 else jnp.where(z >= k, ups[k - 1], downs[line - k - 1])
                        for k in blocks
                    ],
                    axis=0,
                )
                term = lax.dot_general(
                    grads[g].reshape(-1, d_line),
                    chunk,
                    (((0,), (0,)), ((), ())),
                    preferred_element_type=f32,
                )
                product = term if product is None else product + term
            return product * (1.0 / n_dp)

        groups = [sorted({1, line - 1}), [*range(2, line - 1), 0]]
        shifted = []
        for k in [*groups[0], *groups[1]]:
            columns = lax.dynamic_slice(
                upstream, (0, ((z + k) % line) * d_line), (mine, d_line)
            )
            shifted.append(columns if k == 0 else along_line(columns, k))
        block_of = {k: (g, i) for g, blocks in enumerate(groups) for i, k in enumerate(blocks)}

        def gather_grad(g):
            blocks = shifted[: len(groups[0])] if g == 0 else shifted[len(groups[0]) :]
            grad = jnp.stack(blocks)
            got = across_side(grad)
            grad = jnp.stack([grad, got], axis=1)
            got = [along_cross(grad, k) for k in range(1, cross)]
            rolled = jnp.stack([grad] + got)
            swapped = across_core(rolled)
            placed = []
            for to_x in range(cross):
                for to_core in range(2):
                    value = None
                    for k in range(cross):
                        part = jnp.where(core == to_core, rolled[k], swapped[k])
                        value = (
                            part
                            if value is None
                            else jnp.where((x - to_x) % cross == k, part, value)
                        )
                    placed.append(value)
            grad = jnp.stack(placed, axis=2)
            return grad.reshape(len(blocks), 2 * tokens, d_line)

        preact = pre_act.astype(f32)
        activation, slope = lax.optimization_barrier(
            (gelu_exact(preact).astype(bf16), gelu_slope(preact))
        )
        width = half // STREAMS
        keep = lax.dynamic_slice(activation, (0, side * half), (tokens, half))
        give = lax.dynamic_slice(activation, (0, (1 - side) * half), (tokens, half))
        got = across_side(give)
        act = jnp.concatenate([keep, got], axis=0)

        stored_rows = down_weight.shape[0]
        pieces = lax.optimization_barrier(
            [
                lax.dynamic_slice(down_weight, (0, s * half + q * width), (stored_rows, width))
                for q in range(STREAMS)
                for s in (side, 1 - side)
            ]
        )
        got_rows = [across_side(pieces[2 * q + 1]) for q in range(STREAMS)]

        weights, grads, products = [], [], {}

        def multiply(g, q):
            product = lax.dot_general(
                grads[g], weights[q], (((2,), (0,)), ((), ())), preferred_element_type=f32
            )
            products[g, q] = lax.optimization_barrier(product)

        grads.append(gather_grad(0))
        for q in range(STREAMS):
            weights.append(place(pieces[2 * q], got_rows[q], side, 0))
            multiply(0, q)
        grads.append(gather_grad(1))
        for q in range(STREAMS):
            multiply(1, q)

        def part(k, q):
            g, i = block_of[k]
            return products[g, q][i]

        def slot(right, left):
            right = along_line(right, 1, lambda p: p < line - 1)
            left = along_line(left, -1, lambda p: p > 0)
            return right, left

        def of_stream(value, q):
            return value[:, q * width : (q + 1) * width]

        got = slot(act, act)
        moving = [tuple(of_stream(v, q) for v in got) for q in range(STREAMS)]
        ups, downs = [[] for _ in moving], [[] for _ in moving]
        index = side.reshape(1)
        full, others = [], []
        for s in range(2, line + 1):
            for q in range(STREAMS):
                right, left = moving[q]
                ups[q].append(right)
                downs[q].append(left)
                to_right, to_left = part(s - 1, q), part(line - s + 1, q)
                if s == 2 and q:
                    to_right, to_left = first_then(joined, (to_right, to_left))
                right = right.astype(f32) + jnp.where(z < s - 1, to_right, 0.0)
                left = left.astype(f32) + jnp.where(z > line - s, to_left, 0.0)
                joined = right, left = right.astype(bf16), left.astype(bf16)
                if s == line:
                    own_act = of_stream(act, q)
                    if q:
                        own_act, ups[q][0], downs[q][0] = first_then(
                            other, (own_act, ups[q][0], downs[q][0])
                        )
                    product = weight_grad_of(grads, own_act, ups[q], downs[q])
                    other = lax.dynamic_slice(
                        product, ((1 - side) * d_side, 0), (d_side, width)
                    ).astype(bf16)
                    others.append(across_side(other))
                    full.append(product)
                moving[q] = slot(right, left)
        own, gives = [], []
        for q in range(STREAMS):
            def rows_of(low, high):
                terms = [part(0, q), *moving[q]]
                return sum(term[low:high].astype(f32) for term in terms)

            give = rows_of(tokens, 2 * tokens).astype(bf16)
            gives.append(across_side(give))
            own.append(rows_of(0, tokens))
        weight_grad = merge_weight(index, full, others)
        act_grad = merge_act(index, own, gives, slope)

        shares = list(attend(qkv, segment_ids[0], out_weight, t, n_tensor))
        for k in range(1, n_tensor):
            pairs = [(i, (i + k) % n_tensor) for i in range(n_tensor)]
            shares[k] = lax.ppermute(shares[k], "tensor", pairs)
        attention_out = sum(share.astype(f32) for share in shares) + out_bias.astype(f32)
        return (attention_out, act_grad, weight_grad)

    return body


def solution(mesh):
    n_dp, n_tensor = mesh.shape["dp"], mesh.shape["tensor"]
    return jax.shard_map(
        make_body(n_dp, n_tensor),
        mesh=mesh,
        in_specs=(
            P(None, "dp", "tensor"),
            P("dp", None, None),
            P(None, "tensor"),
            P(),
            P(("dp", "tensor"), None),
            P("dp", "tensor"),
            P("dp", "tensor"),
        ),
        out_specs=(P(("dp", "tensor"), None), P("dp", "tensor"), P("dp", "tensor")),
        check_vma=False,
    )
```

```python
import math

import jax
import jax.numpy as jnp
from jax import lax
from jax.experimental import pallas as pl
from jax.experimental.pallas import tpu as pltpu
from jax.sharding import PartitionSpec as P


HEAD = 128
ROWS_DEV = 64


root_half = 1.0 / math.sqrt(2.0)
inv_root_tau = 1.0 / math.sqrt(2.0 * math.pi)
f32, bf16 = jnp.float32, jnp.bfloat16


def gelu_exact(argument):
    return 0.5 * argument * (1.0 + lax.erf(argument * root_half))


def gelu_slope(argument):
    return (
        0.5 * (1.0 + lax.erf(argument * root_half))
        + argument * jnp.exp(-0.5 * argument * argument) * inv_root_tau
    )


def attend_kernel(place_ref, qkv_ref, labels_ref, weight_ref, *refs):
    outs, (context, rolled) = refs[:-2], refs[-2:]
    length, width = context.shape
    share = length // len(outs)

    @pl.when(pl.program_id(0) == 0)
    def _():
        row = jnp.broadcast_to(labels_ref[...].astype(f32), (length, length))
        first = lax.broadcasted_iota(jnp.int32, (length, length), 0) // ROWS_DEV
        second = lax.broadcasted_iota(jnp.int32, (length, length), 1) // ROWS_DEV
        same = (row == row.T) & (first == second)
        for h in range(width // HEAD):
            cols = slice(h * HEAD, (h + 1) * HEAD)
            scores = lax.dot_general(
                qkv_ref[0, :, cols],
                qkv_ref[1, :, cols],
                (((1,), (1,)), ((), ())),
                preferred_element_type=f32,
            ) * (1.0 / math.sqrt(HEAD))
            masked = jnp.where(same, scores, -1e30)
            top = jnp.max(masked, axis=1, keepdims=True)
            exponent = jnp.exp(masked - top)
            inverse = 1.0 / jnp.sum(exponent, axis=1, keepdims=True)
            weights = (exponent * inverse).astype(bf16)
            context[:, cols] = jnp.dot(
                weights, qkv_ref[2, :, cols], preferred_element_type=f32
            ).astype(bf16)
        for k in range(len(outs)):
            start = pl.multiple_of(lax.rem(place_ref[0] + k, len(outs)) * share, share)
            rolled[k * share : (k + 1) * share, :] = context[pl.ds(start, share), :]

    partial = lax.dot_general(
        rolled[...], weight_ref[...], (((1,), (1,)), ((), ())), preferred_element_type=f32
    )
    for k, out in enumerate(outs):
        out[...] = partial[k * share : (k + 1) * share].astype(bf16)


def attend(qkv, labels, out_weight, place, members):
    length, width = qkv.shape[1:]
    d_model = out_weight.shape[0]
    block = min(1024, d_model)
    share = length // members
    grid_spec = pltpu.PrefetchScalarGridSpec(
        num_scalar_prefetch=1,
        grid=(d_model // block,),
        in_specs=[
            pl.BlockSpec(qkv.shape, lambda j, p: (0, 0, 0)),
            pl.BlockSpec((1, length), lambda j, p: (0, 0)),
            pl.BlockSpec((block, width), lambda j, p: (j, 0)),
        ],
        out_specs=[pl.BlockSpec((share, block), lambda j, p: (0, j))] * members,
        scratch_shapes=[pltpu.VMEM((length, width), bf16)] * 2,
    )
    return pl.pallas_call(
        attend_kernel,
        grid_spec=grid_spec,
        out_shape=[jax.ShapeDtypeStruct((share, d_model), bf16)] * members,
        cost_estimate=pl.CostEstimate(
            flops=2 * length * width * (d_model + 2 * length),
            transcendentals=length * length * width // HEAD,
            bytes_accessed=2 * (qkv.size + out_weight.size + length * d_model),
        ),
        name="attend",
    )(place.reshape(1), qkv, labels.reshape(1, length), out_weight)


def merge_weight(index, products, others):
    rows, width = others[0].shape
    streams = len(others)
    steps = max(1, rows // 128)
    step = rows // steps

    def kernel(index_ref, *refs):
        out = refs[-1]
        for q in range(streams):
            mine = refs[q][...]
            theirs = refs[streams + q][...].astype(f32)
            low = slice(q * width, (q + 1) * width)
            high = slice((streams + q) * width, (streams + q + 1) * width)

            @pl.when(index_ref[0] == 0)
            def _():
                out[:, low] = mine
                out[:, high] = theirs

            @pl.when(index_ref[0] != 0)
            def _():
                out[:, low] = theirs
                out[:, high] = mine

    return pl.pallas_call(
        kernel,
        grid_spec=pltpu.PrefetchScalarGridSpec(
            num_scalar_prefetch=1,
            grid=(steps,),
            in_specs=[pl.BlockSpec((step, width), lambda i, n: (n[0] * steps + i, 0))] * streams
            + [pl.BlockSpec((step, width), lambda i, n: (i, 0))] * streams,
            out_specs=pl.BlockSpec((step, 2 * streams * width), lambda i, n: (i, 0)),
        ),
        out_shape=jax.ShapeDtypeStruct((rows, 2 * streams * width), f32),
        name="merge_weight",
    )(index, *products, *others)


def merge_act(index, own, others, slope):
    rows, width = others[0].shape
    streams = len(others)
    steps = max(1, rows // 128)
    step = rows // steps

    def kernel(index_ref, *refs):
        factor, out = refs[-2], refs[-1]
        for q in range(streams):
            mine = refs[q][...]
            theirs = refs[streams + q][...].astype(f32)
            low = slice(q * width, (q + 1) * width)
            high = slice((streams + q) * width, (streams + q + 1) * width)

            @pl.when(index_ref[0] == 0)
            def _():
                out[:, low] = mine * factor[:, low]
                out[:, high] = theirs * factor[:, high]

            @pl.when(index_ref[0] != 0)
            def _():
                out[:, low] = theirs * factor[:, low]
                out[:, high] = mine * factor[:, high]

    block = pl.BlockSpec((step, width), lambda i, n: (i, 0))
    wide = pl.BlockSpec((step, 2 * streams * width), lambda i, n: (i, 0))
    return pl.pallas_call(
        kernel,
        grid_spec=pltpu.PrefetchScalarGridSpec(
            num_scalar_prefetch=1,
            grid=(steps,),
            in_specs=[block] * (2 * streams) + [wide],
            out_specs=wide,
        ),
        out_shape=jax.ShapeDtypeStruct(slope.shape, f32),
        name="merge_act",
    )(index, *own, *others, slope)


STREAMS = 2


def make_body(n_dp, n_tensor):
    line, cross = n_dp // 2, n_tensor // 2

    def along_line(value, shift, keep=lambda z: True):
        pairs = []
        for z in range(line):
            if keep(z):
                for side in range(2):
                    pairs.append((2 * z + side, 2 * ((z + shift) % line) + side))
        return lax.ppermute(value, "dp", pairs)

    def across_side(value):
        return lax.ppermute(value, "dp", [(i, i ^ 1) for i in range(n_dp)])

    def across_core(value):
        return lax.ppermute(value, "tensor", [(t, t ^ 1) for t in range(n_tensor)])

    def along_cross(value, shift):
        return lax.ppermute(
            value, "tensor", [(t, (t + 2 * shift) % n_tensor) for t in range(n_tensor)]
        )

    def place(own, other, index, axis):
        first = jnp.where(index == 0, own, other)
        second = jnp.where(index == 0, other, own)
        return jnp.concatenate([first, second], axis=axis)

    def body(qkv, segment_ids, out_weight, out_bias, upstream, pre_act, down_weight):
        dp = lax.axis_index("dp")
        z, side = dp // 2, dp % 2
        t = lax.axis_index("tensor")
        x, core = t // 2, t % 2
        mine, d_model = upstream.shape
        tokens, hidden = pre_act.shape
        d_line = d_model // line
        d_side = d_line // 2
        half = hidden // 2

        def first_then(first, then):
            return lax.optimization_barrier((then, first))[0]

        def weight_grad_of(grads, act, ups, downs):
            product = None
            for g, blocks in enumerate(groups):
                chunk = jnp.concatenate(
                    [
                        act if k == 0 else jnp.where(z >= k, ups[k - 1], downs[line - k - 1])
                        for k in blocks
                    ],
                    axis=0,
                )
                term = lax.dot_general(
                    grads[g].reshape(-1, d_line),
                    chunk,
                    (((0,), (0,)), ((), ())),
                    preferred_element_type=f32,
                )
                product = term if product is None else product + term
            return product * (1.0 / n_dp)

        groups = [sorted({1, line - 1}), [*range(2, line - 1), 0]]
        shifted = []
        for k in [*groups[0], *groups[1]]:
            columns = lax.dynamic_slice(
                upstream, (0, ((z + k) % line) * d_line), (mine, d_line)
            )
            shifted.append(columns if k == 0 else along_line(columns, k))
        block_of = {k: (g, i) for g, blocks in enumerate(groups) for i, k in enumerate(blocks)}

        def gather_grad(g):
            blocks = shifted[: len(groups[0])] if g == 0 else shifted[len(groups[0]) :]
            grad = jnp.stack(blocks)
            got = across_side(grad)
            grad = jnp.stack([grad, got], axis=1)
            got = [along_cross(grad, k) for k in range(1, cross)]
            rolled = jnp.stack([grad] + got)
            swapped = across_core(rolled)
            placed = []
            for to_x in range(cross):
                for to_core in range(2):
                    value = None
                    for k in range(cross):
                        part = jnp.where(core == to_core, rolled[k], swapped[k])
                        value = (
                            part
                            if value is None
                            else jnp.where((x - to_x) % cross == k, part, value)
                        )
                    placed.append(value)
            grad = jnp.stack(placed, axis=2)
            return grad.reshape(len(blocks), 2 * tokens, d_line)

        width = half // STREAMS
        given = lax.dynamic_slice(pre_act, (0, (1 - side) * half), (tokens, half)).astype(f32)
        give = lax.optimization_barrier(gelu_exact(given).astype(bf16))
        preact = pre_act.astype(f32)
        kept = lax.dynamic_slice(preact, (0, side * half), (tokens, half))
        keep, slope = lax.optimization_barrier((gelu_exact(kept).astype(bf16), gelu_slope(preact)))
        got = across_side(give)
        act = jnp.concatenate([keep, got], axis=0)

        stored_rows = down_weight.shape[0]
        pieces = lax.optimization_barrier(
            [
                lax.dynamic_slice(down_weight, (0, s * half + q * width), (stored_rows, width))
                for q in range(STREAMS)
                for s in (side, 1 - side)
            ]
        )
        got_rows = [across_side(pieces[2 * q + 1]) for q in range(STREAMS)]

        weights, grads, products = [], [], {}

        def multiply(g, q):
            product = lax.dot_general(
                grads[g], weights[q], (((2,), (0,)), ((), ())), preferred_element_type=f32
            )
            products[g, q] = lax.optimization_barrier(product)

        grads.append(gather_grad(0))
        for q in range(STREAMS):
            weights.append(place(pieces[2 * q], got_rows[q], side, 0))
            multiply(0, q)
        grads.append(gather_grad(1))
        for q in range(STREAMS):
            multiply(1, q)

        def part(k, q):
            g, i = block_of[k]
            return products[g, q][i]

        def slot(right, left):
            right = along_line(right, 1, lambda p: p < line - 1)
            left = along_line(left, -1, lambda p: p > 0)
            return right, left

        def of_stream(value, q):
            return value[:, q * width : (q + 1) * width]

        got = slot(act, act)
        moving = [tuple(of_stream(v, q) for v in got) for q in range(STREAMS)]
        ups, downs = [[] for _ in moving], [[] for _ in moving]
        index = side.reshape(1)
        full, others = [], []
        for s in range(2, line + 1):
            for q in range(STREAMS):
                right, left = moving[q]
                ups[q].append(right)
                downs[q].append(left)
                to_right, to_left = part(s - 1, q), part(line - s + 1, q)
                if s == 2 and q:
                    to_right, to_left = first_then(joined, (to_right, to_left))
                right = right.astype(f32) + jnp.where(z < s - 1, to_right, 0.0)
                left = left.astype(f32) + jnp.where(z > line - s, to_left, 0.0)
                joined = right, left = right.astype(bf16), left.astype(bf16)
                if s == line:
                    own_act = of_stream(act, q)
                    if q:
                        own_act, ups[q][0], downs[q][0] = first_then(
                            other, (own_act, ups[q][0], downs[q][0])
                        )
                    product = weight_grad_of(grads, own_act, ups[q], downs[q])
                    other = lax.dynamic_slice(
                        product, ((1 - side) * d_side, 0), (d_side, width)
                    ).astype(bf16)
                    others.append(across_side(other))
                    full.append(product)
                moving[q] = slot(right, left)
        own, gives = [], []
        for q in range(STREAMS):
            def rows_of(low, high):
                terms = [part(0, q), *moving[q]]
                return sum(term[low:high].astype(f32) for term in terms)

            give = rows_of(tokens, 2 * tokens).astype(bf16)
            gives.append(across_side(give))
            own.append(rows_of(0, tokens))
        weight_grad = merge_weight(index, full, others)
        act_grad = merge_act(index, own, gives, slope)

        shares = list(attend(qkv, segment_ids[0], out_weight, t, n_tensor))
        for k in range(1, n_tensor):
            pairs = [(i, (i + k) % n_tensor) for i in range(n_tensor)]
            shares[k] = lax.ppermute(shares[k], "tensor", pairs)
        attention_out = sum(share.astype(f32) for share in shares) + out_bias.astype(f32)
        return (attention_out, act_grad, weight_grad)

    return body


def solution(mesh):
    n_dp, n_tensor = mesh.shape["dp"], mesh.shape["tensor"]
    return jax.shard_map(
        make_body(n_dp, n_tensor),
        mesh=mesh,
        in_specs=(
            P(None, "dp", "tensor"),
            P("dp", None, None),
            P(None, "tensor"),
            P(),
            P(("dp", "tensor"), None),
            P("dp", "tensor"),
            P("dp", "tensor"),
        ),
        out_specs=(P(("dp", "tensor"), None), P("dp", "tensor"), P("dp", "tensor")),
        check_vma=False,
    )
```

```python
import math

import jax
import jax.numpy as jnp
from jax import lax
from jax.experimental import pallas as pl
from jax.experimental.pallas import tpu as pltpu
from jax.sharding import PartitionSpec as P


HEAD = 128
ROWS_DEV = 64


root_half = 1.0 / math.sqrt(2.0)
inv_root_tau = 1.0 / math.sqrt(2.0 * math.pi)
f32, bf16 = jnp.float32, jnp.bfloat16


def gelu_exact(argument):
    return 0.5 * argument * (1.0 + lax.erf(argument * root_half))


def gelu_slope(argument):
    return (
        0.5 * (1.0 + lax.erf(argument * root_half))
        + argument * jnp.exp(-0.5 * argument * argument) * inv_root_tau
    )


def attend_kernel(place_ref, qkv_ref, labels_ref, weight_ref, *refs):
    outs, (context, rolled) = refs[:-2], refs[-2:]
    length, width = context.shape
    share = length // len(outs)

    @pl.when(pl.program_id(0) == 0)
    def _():
        row = jnp.broadcast_to(labels_ref[...].astype(f32), (length, length))
        first = lax.broadcasted_iota(jnp.int32, (length, length), 0) // ROWS_DEV
        second = lax.broadcasted_iota(jnp.int32, (length, length), 1) // ROWS_DEV
        same = (row == row.T) & (first == second)
        for h in range(width // HEAD):
            cols = slice(h * HEAD, (h + 1) * HEAD)
            scores = lax.dot_general(
                qkv_ref[0, :, cols],
                qkv_ref[1, :, cols],
                (((1,), (1,)), ((), ())),
                preferred_element_type=f32,
            ) * (1.0 / math.sqrt(HEAD))
            masked = jnp.where(same, scores, -1e30)
            top = jnp.max(masked, axis=1, keepdims=True)
            exponent = jnp.exp(masked - top)
            inverse = 1.0 / jnp.sum(exponent, axis=1, keepdims=True)
            weights = (exponent * inverse).astype(bf16)
            context[:, cols] = jnp.dot(
                weights, qkv_ref[2, :, cols], preferred_element_type=f32
            ).astype(bf16)
        for k in range(len(outs)):
            start = pl.multiple_of(lax.rem(place_ref[0] + k, len(outs)) * share, share)
            rolled[k * share : (k + 1) * share, :] = context[pl.ds(start, share), :]

    partial = lax.dot_general(
        rolled[...], weight_ref[...], (((1,), (1,)), ((), ())), preferred_element_type=f32
    )
    for k, out in enumerate(outs):
        out[...] = partial[k * share : (k + 1) * share].astype(bf16)


def attend(qkv, labels, out_weight, place, members):
    length, width = qkv.shape[1:]
    d_model = out_weight.shape[0]
    block = min(2048, d_model)
    share = length // members
    grid_spec = pltpu.PrefetchScalarGridSpec(
        num_scalar_prefetch=1,
        grid=(d_model // block,),
        in_specs=[
            pl.BlockSpec(qkv.shape, lambda j, p: (0, 0, 0)),
            pl.BlockSpec((1, length), lambda j, p: (0, 0)),
            pl.BlockSpec((block, width), lambda j, p: (j, 0)),
        ],
        out_specs=[pl.BlockSpec((share, block), lambda j, p: (0, j))] * members,
        scratch_shapes=[pltpu.VMEM((length, width), bf16)] * 2,
    )
    return pl.pallas_call(
        attend_kernel,
        grid_spec=grid_spec,
        out_shape=[jax.ShapeDtypeStruct((share, d_model), bf16)] * members,
        cost_estimate=pl.CostEstimate(
            flops=2 * length * width * (d_model + 2 * length),
            transcendentals=length * length * width // HEAD,
            bytes_accessed=2 * (qkv.size + out_weight.size + length * d_model),
        ),
        name="attend",
    )(place.reshape(1), qkv, labels.reshape(1, length), out_weight)


def merge_weight(index, products, others):
    rows, width = others[0].shape
    streams = len(others)
    steps = max(1, rows // 256)
    step = rows // steps

    def kernel(index_ref, *refs):
        out = refs[-1]
        for q in range(streams):
            mine = refs[q][...]
            theirs = refs[streams + q][...].astype(f32)
            low = slice(q * width, (q + 1) * width)
            high = slice((streams + q) * width, (streams + q + 1) * width)

            @pl.when(index_ref[0] == 0)
            def _():
                out[:, low] = mine
                out[:, high] = theirs

            @pl.when(index_ref[0] != 0)
            def _():
                out[:, low] = theirs
                out[:, high] = mine

    return pl.pallas_call(
        kernel,
        grid_spec=pltpu.PrefetchScalarGridSpec(
            num_scalar_prefetch=1,
            grid=(steps,),
            in_specs=[pl.BlockSpec((step, width), lambda i, n: (n[0] * steps + i, 0))] * streams
            + [pl.BlockSpec((step, width), lambda i, n: (i, 0))] * streams,
            out_specs=pl.BlockSpec((step, 2 * streams * width), lambda i, n: (i, 0)),
        ),
        out_shape=jax.ShapeDtypeStruct((rows, 2 * streams * width), f32),
        name="merge_weight",
    )(index, *products, *others)


def merge_act(index, sources, slope, buffer):
    rows, width = sources[0][0].shape
    streams = slope.shape[1] // (2 * width)
    count = len(sources)

    def column(j, n):
        block = 0
        for m, (_, sent, q) in enumerate(sources):
            half = 1 - n[0] if sent else n[0]
            block = jnp.where(j == m, half * streams + q, block)
        return block

    def kernel(index_ref, *refs):
        factor, out = refs[count], refs[-1]
        for m in range(count):

            @pl.when(pl.program_id(0) == m)
            def _():
                out[...] = refs[m][...].astype(f32) * factor[...]

    target = pl.BlockSpec((rows, width), lambda j, n: (0, column(j, n)))
    operands = [index] + [array for array, _, _ in sources] + [slope]
    in_specs = [pl.BlockSpec((rows, width), lambda j, n: (0, 0))] * count + [target]
    aliases = {}
    if buffer is not None:
        aliases = {len(operands): 0}
        operands.append(buffer)
        in_specs.append(pl.BlockSpec(memory_space=pl.ANY))
    return pl.pallas_call(
        kernel,
        grid_spec=pltpu.PrefetchScalarGridSpec(
            num_scalar_prefetch=1, grid=(count,), in_specs=in_specs, out_specs=target
        ),
        out_shape=jax.ShapeDtypeStruct(slope.shape, f32),
        input_output_aliases=aliases,
        name="merge_act",
    )(*operands)


STREAMS = 2


def make_body(n_dp, n_tensor):
    line, cross = n_dp // 2, n_tensor // 2

    def along_line(value, shift, keep=lambda z: True):
        pairs = []
        for z in range(line):
            if keep(z):
                for side in range(2):
                    pairs.append((2 * z + side, 2 * ((z + shift) % line) + side))
        return lax.ppermute(value, "dp", pairs)

    def across_side(value):
        return lax.ppermute(value, "dp", [(i, i ^ 1) for i in range(n_dp)])

    def across_core(value):
        return lax.ppermute(value, "tensor", [(t, t ^ 1) for t in range(n_tensor)])

    def along_cross(value, shift):
        return lax.ppermute(
            value, "tensor", [(t, (t + 2 * shift) % n_tensor) for t in range(n_tensor)]
        )

    def place(own, other, index, axis):
        first = jnp.where(index == 0, own, other)
        second = jnp.where(index == 0, other, own)
        return jnp.concatenate([first, second], axis=axis)

    def body(qkv, segment_ids, out_weight, out_bias, upstream, pre_act, down_weight):
        dp = lax.axis_index("dp")
        z, side = dp // 2, dp % 2
        t = lax.axis_index("tensor")
        x, core = t // 2, t % 2
        mine, d_model = upstream.shape
        tokens, hidden = pre_act.shape
        d_line = d_model // line
        d_side = d_line // 2
        half = hidden // 2

        def first_then(first, then):
            return lax.optimization_barrier((then, first))[0]

        def weight_grad_of(grads, act, ups, downs):
            product = None
            for g, blocks in enumerate(groups):
                chunk = jnp.concatenate(
                    [
                        act if k == 0 else jnp.where(z >= k, ups[k - 1], downs[line - k - 1])
                        for k in blocks
                    ],
                    axis=0,
                )
                term = lax.dot_general(
                    grads[g].reshape(-1, d_line),
                    chunk,
                    (((0,), (0,)), ((), ())),
                    preferred_element_type=f32,
                )
                product = term if product is None else product + term
            return product * (1.0 / n_dp)

        groups = [sorted({1, line - 1}), [*range(2, line - 1), 0]]
        shifted = []
        for k in [*groups[0], *groups[1]]:
            columns = lax.dynamic_slice(
                upstream, (0, ((z + k) % line) * d_line), (mine, d_line)
            )
            shifted.append(columns if k == 0 else along_line(columns, k))
        block_of = {k: (g, i) for g, blocks in enumerate(groups) for i, k in enumerate(blocks)}

        def gather_grad(g):
            blocks = shifted[: len(groups[0])] if g == 0 else shifted[len(groups[0]) :]
            grad = jnp.stack(blocks)
            got = across_side(grad)
            grad = jnp.stack([grad, got], axis=1)
            got = [along_cross(grad, k) for k in range(1, cross)]
            rolled = jnp.stack([grad] + got)
            swapped = across_core(rolled)
            placed = []
            for to_x in range(cross):
                for to_core in range(2):
                    value = None
                    for k in range(cross):
                        part = jnp.where(core == to_core, rolled[k], swapped[k])
                        value = (
                            part
                            if value is None
                            else jnp.where((x - to_x) % cross == k, part, value)
                        )
                    placed.append(value)
            grad = jnp.stack(placed, axis=2)
            return grad.reshape(len(blocks), 2 * tokens, d_line)

        width = half // STREAMS
        given = lax.dynamic_slice(pre_act, (0, (1 - side) * half), (tokens, half)).astype(f32)
        give = lax.optimization_barrier(gelu_exact(given).astype(bf16))
        preact = pre_act.astype(f32)
        kept = lax.dynamic_slice(preact, (0, side * half), (tokens, half))
        keep, slope = lax.optimization_barrier((gelu_exact(kept).astype(bf16), gelu_slope(preact)))
        got = across_side(give)
        act = jnp.concatenate([keep, got], axis=0)

        stored_rows = down_weight.shape[0]
        pieces = lax.optimization_barrier(
            [
                lax.dynamic_slice(down_weight, (0, s * half + q * width), (stored_rows, width))
                for q in range(STREAMS)
                for s in (side, 1 - side)
            ]
        )
        got_rows = [across_side(pieces[2 * q + 1]) for q in range(STREAMS)]

        weights, grads, products = [], [], {}

        def multiply(g, q):
            product = lax.dot_general(
                grads[g], weights[q], (((2,), (0,)), ((), ())), preferred_element_type=f32
            )
            products[g, q] = lax.optimization_barrier(product)

        grads.append(gather_grad(0))
        for q in range(STREAMS):
            weights.append(place(pieces[2 * q], got_rows[q], side, 0))
            multiply(0, q)
        grads.append(gather_grad(1))
        for q in range(STREAMS):
            multiply(1, q)

        def part(k, q):
            g, i = block_of[k]
            return products[g, q][i]

        def slot(right, left):
            right = along_line(right, 1, lambda p: p < line - 1)
            left = along_line(left, -1, lambda p: p > 0)
            return right, left

        def of_stream(value, q):
            return value[:, q * width : (q + 1) * width]

        got = slot(act, act)
        moving = [tuple(of_stream(v, q) for v in got) for q in range(STREAMS)]
        ups, downs = [[] for _ in moving], [[] for _ in moving]
        index = side.reshape(1)
        full, others = [], []
        for s in range(2, line + 1):
            for q in range(STREAMS):
                right, left = moving[q]
                ups[q].append(right)
                downs[q].append(left)
                to_right, to_left = part(s - 1, q), part(line - s + 1, q)
                if s == 2 and q:
                    to_right, to_left = first_then(joined, (to_right, to_left))
                right = right.astype(f32) + jnp.where(z < s - 1, to_right, 0.0)
                left = left.astype(f32) + jnp.where(z > line - s, to_left, 0.0)
                joined = right, left = right.astype(bf16), left.astype(bf16)
                if s == line:
                    own_act = of_stream(act, q)
                    if q:
                        own_act, ups[q][0], downs[q][0] = first_then(
                            other, (own_act, ups[q][0], downs[q][0])
                        )
                    product = weight_grad_of(grads, own_act, ups[q], downs[q])
                    other = lax.dynamic_slice(
                        product, ((1 - side) * d_side, 0), (d_side, width)
                    ).astype(bf16)
                    others.append(across_side(other))
                    full.append(product)
                moving[q] = slot(right, left)
        own, gives = [], []
        for q in range(STREAMS):
            terms = [part(0, q), *moving[q]]
            give = sum(term[tokens:].astype(f32) for term in terms).astype(bf16)
            gives.append(across_side(give))
            terms = first_then(give, terms)
            own.append(sum(term[:tokens].astype(f32) for term in terms))
        weight_grad = merge_weight(index, full, others)
        early = [(h, False, q) for q, h in enumerate(own)]
        early += [(h, True, q) for q, h in enumerate(gives[:-1])]
        act_grad = merge_act(index, early, slope, None)
        act_grad = merge_act(index, [(gives[-1], True, STREAMS - 1)], slope, act_grad)

        shares = list(attend(qkv, segment_ids[0], out_weight, t, n_tensor))
        for k in range(1, n_tensor):
            pairs = [(i, (i + k) % n_tensor) for i in range(n_tensor)]
            shares[k] = lax.ppermute(shares[k], "tensor", pairs)
        attention_out = sum(share.astype(f32) for share in shares) + out_bias.astype(f32)
        return (attention_out, act_grad, weight_grad)

    return body


def solution(mesh):
    n_dp, n_tensor = mesh.shape["dp"], mesh.shape["tensor"]
    return jax.shard_map(
        make_body(n_dp, n_tensor),
        mesh=mesh,
        in_specs=(
            P(None, "dp", "tensor"),
            P("dp", None, None),
            P(None, "tensor"),
            P(),
            P(("dp", "tensor"), None),
            P("dp", "tensor"),
            P("dp", "tensor"),
        ),
        out_specs=(P(("dp", "tensor"), None), P("dp", "tensor"), P("dp", "tensor")),
        check_vma=False,
    )
```
